32 devices in a mesh: rep: 2 (over x), dp: 16 (over y, z, core).
Axes of the slice: x: 2, y: 2, z: 4, core: 2. Of those that a mesh axis runs over, the one named last changes fastest.
Arguments:
- x: bfloat16 [32, 4096, 512], P(('rep', 'dp')), parts along dimension 0
- dy: bfloat16 [32, 4096, 512], P(('rep', 'dp')), parts along dimension 0
- w_gate: bfloat16 [2, 512, 2048], P(None, 'dp')
- w_up: bfloat16 [2, 512, 2048], P(None, 'dp')
- w_down: bfloat16 [2, 2048, 512], P(None, 'dp')
Outputs:
- output 1: bfloat16 [32, 4096, 512], P(('rep', 'dp')), parts along dimension 0
- output 2: bfloat16 [4, 512, 2048], P('rep', 'dp'), parts along dimension 0
- output 3: bfloat16 [4, 512, 2048], P('rep', 'dp'), parts along dimension 0
- output 4: bfloat16 [4, 2048, 512], P('rep', 'dp'), parts along dimension 0
There are 2 independent parts. The reference program is written for one: setup_inputs(seed, part) draws one part's arguments, and reference() takes and returns one part's arrays. A program takes and returns all parts, laid end to end along the dimension named above; an argument that names none is the same for every part.
All inputs are finite; a program needn't handle non-finite values.
Results may differ from the reference program's by a relative error of at most 0.018.
Values are sent between devices in bfloat16 or wider.
A program may use at most 2 GiB of HBM per device.

```python
import jax
import jax.numpy as jnp
from jax import lax

SEQUENCES = 16
TOKENS = 4096
D = 512
FF = 2048
LAYERS = 2
NAMES = ("w_gate", "w_up", "w_down")
SHAPES = {"w_gate": (LAYERS, D, FF), "w_up": (LAYERS, D, FF), "w_down": (LAYERS, FF, D)}


def bump(key, n, height):
    away = (jnp.arange(n, dtype=jnp.int32) - jax.random.randint(key, (), 0, n, jnp.int32)) % n
    return jnp.where(away < n // 8, height, 1.0)


def together(key, own, strength):
    shared = jax.random.normal(key, own.shape[1:], jnp.float32)
    return (own + strength * shared) * lax.rsqrt(1 + strength * strength)


def setup_inputs(seed: int = 0, part: int = 0) -> dict:
    kx, kdy, ka, kb, kz, kf, kh, kl, *kw = jax.random.split(jax.random.key(seed), 8 + len(NAMES))
    kx, kdy, ka, kb = (jax.random.fold_in(k, part) for k in (kx, kdy, ka, kb))
    shape = (SEQUENCES, TOKENS, D)
    much_x, much_dy = jax.random.uniform(kz, (2,), jnp.float32, 0.0, 1.0)
    layers = 2.0 ** jax.random.uniform(kl, (LAYERS, 1, 1), jnp.float32, -1.0, 1.0)
    x = together(ka, jax.random.normal(kx, shape, jnp.float32), much_x) * bump(kf, D, 4.0)
    dy = together(kb, jax.random.normal(kdy, shape, jnp.float32), much_dy)
    drawn = {"x": x.astype(jnp.bfloat16), "dy": (dy * (SEQUENCES * TOKENS) ** -0.5).astype(jnp.bfloat16)}
    for key, name in zip(kw, NAMES, strict=True):
        w = jax.random.normal(key, SHAPES[name], jnp.float32) * SHAPES[name][1] ** -0.5
        drawn[name] = (w * {"w_gate": 1.0, "w_up": bump(kh, FF, 4.0), "w_down": layers}[name]).astype(jnp.bfloat16)
    return drawn


def matmul(a, w):
    return jnp.dot(a, w, preferred_element_type=jnp.float32).astype(jnp.bfloat16)


def normed(h):
    wide = h.astype(jnp.float32)
    scale = lax.rsqrt(jnp.mean(wide**2, -1, keepdims=True) + 1e-6)
    return (wide * scale).astype(jnp.bfloat16)


def layer(h, w):
    a = normed(h)
    gate = jnp.dot(a, w["w_gate"], preferred_element_type=jnp.float32)
    up = jnp.dot(a, w["w_up"], preferred_element_type=jnp.float32)
    return h + matmul((jax.nn.silu(gate) * up).astype(jnp.bfloat16), w["w_down"])


def stack(weights, h):
    return lax.scan(lambda h, w: (layer(h, w), None), h, weights)[0]


def reference(x, dy, w_gate, w_up, w_down):
    weights = dict(zip(NAMES, (w_gate, w_up, w_down), strict=True))

    def take(so_far, sequence):
        h, by_y = sequence
        _, back = jax.vjp(stack, weights, h)
        by_weights, by_h = back(by_y)
        return jax.tree.map(lambda total, term: total + term.astype(jnp.float32), so_far, by_weights), by_h

    none_yet = {name: jnp.zeros(w.shape, jnp.float32) for name, w in weights.items()}
    by_weights, by_x = lax.scan(take, none_yet, (x, dy))
    return (by_x, *(by_weights[name].astype(jnp.bfloat16) for name in NAMES))
```

```python
import functools

import jax
import jax.numpy as jnp
from jax import lax
from jax.experimental import pallas as pl
from jax.experimental.pallas import tpu as pltpu
from jax.sharding import PartitionSpec as P

MESH = pl.DeviceIdType.MESH
Y, Z, C = 2, 4, 2
NJ = 4
NT = 4
NQ = 4
bf, f32 = jnp.bfloat16, jnp.float32


def mm(a, b):
    return jnp.dot(a, b, preferred_element_type=f32)


def sigmoid(v):
    return 0.5 * jnp.tanh(0.5 * v) + 0.5


def scale_of(wide):
    return lax.rsqrt(jnp.mean(wide * wide, -1, keepdims=True) + 1e-6)


def kernel(x, dy, wg, wu, wd, dx, owg, owu, owd, h1, G, W, A, AT, DO, DOT, ACC, ag, au, ad, act_s, dgu, wt, wdt,
           P1g, P1w, Q1g, Q1w, P2g, P2w, Q2g, Q2w, K1g, K1w, P3g, P3w, K2g, K2w, Q3g, Q3w, Og, Ow,
           own_sem, tile_sem, tile2_sem, ags, agr, rss, rsr, out_sem, outw_sem):
    L = wg.shape[0]
    T, D = A.shape
    H = act_s
    TM = T // NT
    SUB = TM // 2
    R = wg.shape[1]
    FR = wd.shape[1]
    FC = NJ * FR
    HC = FC // 2
    me = lax.axis_index("dp")
    y, z, c = me // (Z * C), (me // C) % Z, me % C

    def dp(yy, zz, cc):
        return {"dp": (yy * Z + zz) * C + cc}

    partner, ypeer = dp(y, z, 1 - c), dp(1 - y, z, c)

    def zx(k):
        hi, lo = z // 2, z % 2
        if k & 2:
            hi = 1 - hi
        if k & 1:
            lo = 1 - lo
        return hi * 2 + lo

    zpeer = [None] + [dp(y, zx(k), c) for k in (1, 2, 3)]
    jmap = lambda i: i + 1 - 2 * (i % 2)

    def remote(src, dst, ss, rs, dev):
        return pltpu.make_async_remote_copy(src_ref=src, dst_ref=dst, send_sem=ss, recv_sem=rs, device_id=dev, device_id_type=MESH)

    def li(u):
        return u // NJ, jmap(u % NJ)

    def own_copies(l):
        out = []
        for j in range(NJ):
            for g, w in enumerate((wg, wu)):
                for h in range(2):
                    out.append(pltpu.make_async_copy(
                        w.at[l, :, pl.ds(h * (FC * 2) + j * HC, HC)], G.at[l, j, g, y, z, c, :, pl.ds(h * HC, HC)],
                        own_sem.at[l, (j * 2 + g) * 2 + h]))
        out.append(pltpu.make_async_copy(wd.at[l], W.at[l, z, y, c], own_sem.at[l, NJ * 4]))
        return out

    def g_piece(u, zz):
        l, j = li(u)
        ref = G.at[l, j, :, y, zz, c]
        return ref

    def ag_z(u, k):
        l, j = li(u)
        ref = G.at[l, j, :, y, z, c]
        return remote(ref, ref, ags.at[u, k - 1], agr.at[u, k - 1], zpeer[k])

    def ag_z_in(u, k):
        l, j = li(u)
        ref = G.at[l, j, :, y, zx(k), c]
        return remote(ref, ref, ags.at[u, k - 1], agr.at[u, k - 1], zpeer[k])

    def ag_zw(u, k):
        l, j = li(u)
        ref = W.at[l, j, y, c]
        return remote(ref, ref, ags.at[u, 2 + k], agr.at[u, 3], zpeer[k])

    def ag_y(u, k):
        l, j = li(u)
        ref = G.at[l, j, :, y, zx(k), c]
        return remote(ref, ref, ags.at[u, 6 + k], agr.at[u, 4 + k], ypeer)

    def ag_y_in(u, k):
        l, j = li(u)
        ref = G.at[l, j, :, 1 - y, zx(k), c]
        return remote(ref, ref, ags.at[u, 6 + k], agr.at[u, 4 + k], ypeer)

    def ag_yw(u, yy):
        l, j = li(u)
        ref = W.at[l, j, yy, c]
        return remote(ref, ref, ags.at[u, 10], agr.at[u, 8], ypeer)

    def ag_p(u, cc):
        l, j = li(u)
        ref = G.at[l, j, :, :, :, cc]
        return remote(ref, ref, ags.at[u, 11], agr.at[u, 9], partner)

    def ag_pw(u, cc):
        l, j = li(u)
        ref = W.at[l, j, :, cc]
        return remote(ref, ref, ags.at[u, 12], agr.at[u, 10], partner)

    def R1(u):
        l, j = li(u)
        for k in (1, 2, 3):
            ag_z(u, k).start()
        ag_y(u, 0).start()

        @pl.when(z == j)
        def _():
            for k in (1, 2, 3):
                ag_zw(u, k).start()
            ag_yw(u, y).start()

    def E(u, k):
        l, j = li(u)
        ag_z_in(u, k).wait_recv()
        ag_y(u, k).start()

    def Ew(u):
        l, j = li(u)

        @pl.when(z != j)
        def _():
            ag_zw(u, 1).wait_recv()
            ag_yw(u, y).start()

    def E4(u):
        for k in range(4):
            ag_y_in(u, k).wait_recv()
        ag_yw(u, 1 - y).wait_recv()
        ag_p(u, c).start()
        ag_pw(u, c).start()

    def E5(u):
        ag_p(u, 1 - c).wait_recv()
        ag_pw(u, 1 - c).wait_recv()

    def ag_finish(u):
        l, j = li(u)
        for k in (1, 2, 3):
            ag_z(u, k).wait_send()
        for k in range(4):
            ag_y(u, k).wait_send()

        @pl.when(z == j)
        def _():
            for k in (1, 2, 3):
                ag_zw(u, k).wait_send()
        ag_yw(u, y).wait_send()
        ag_p(u, c).wait_send()
        ag_pw(u, c).wait_send()

    def vl(v):
        return L - 1 - v // NJ, jmap(v % NJ)

    def s1(v):
        b = v % 2
        return (remote(P1g, Q1g.at[b], rss.at[0], rsr.at[b, 0], partner), remote(P1w, Q1w.at[b], rss.at[1], rsr.at[b, 1], partner))

    def s2(v):
        b = v % 2
        return (remote(P2g, Q2g.at[b], rss.at[2], rsr.at[b, 2], ypeer), remote(P2w, Q2w.at[b], rss.at[3], rsr.at[b, 3], ypeer))

    def s3(v, k):
        b = v % 2
        return remote(P3g.at[k], Q3g.at[b, k - 1], rss.at[3 + k], rsr.at[b, 3 + k], zpeer[k])

    def s3w(v, k):
        b = v % 2
        return remote(P3w, Q3w.at[k - 1], rss.at[7], rsr.at[b, 6 + k], zpeer[k])

    def wrows(yy, cc):
        return pl.ds(pl.multiple_of((yy * C + cc) * FR, FR), FR)

    def S1(v):
        @pl.when(v > 0)
        def _():
            for d in s1(v - 1):
                d.wait_send()
        for g, acc in enumerate((ag, au)):
            P1g[g] = acc[:, :, 1 - c].astype(bf)
        ad[...] = ad[...].T
        for yy in range(Y):
            P1w[yy] = ad[wrows(yy, 1 - c), :].astype(bf)
        for d in s1(v):
            d.start()

    def A1S2(v):
        b = v % 2
        for d in s1(v):
            d.wait_recv()

        @pl.when(v > 0)
        def _():
            for d in s2(v - 1):
                d.wait_send()
        for g, acc in enumerate((ag, au)):
            K1g[g] = acc[y, :, c] + Q1g[b, g, y].astype(f32)
            P2g[g] = (acc[1 - y, :, c] + Q1g[b, g, 1 - y].astype(f32)).astype(bf)
        K1w[...] = ad[wrows(y, c), :] + Q1w[b, y].astype(f32)
        P2w[...] = (ad[wrows(1 - y, c), :] + Q1w[b, 1 - y].astype(f32)).astype(bf)
        for d in s2(v):
            d.start()

    def s3_sent(v):
        l, j = vl(v)
        for k in (1, 2, 3):
            s3(v, k).wait_send()

        @pl.when(z != j)
        def _():
            s3w(v, 1).wait_send()

    def A2S3(v):
        l, j = vl(v)
        b = v % 2
        for d in s2(v):
            d.wait_recv()

        @pl.when(v > 0)
        def _():
            s3_sent(v - 1)
        for k in range(4):
            t = K1g[:, zx(k)] + Q2g[b, :, zx(k)].astype(f32)
            if k == 0:
                K2g[...] = t
            else:
                P3g[k] = t.astype(bf)
                s3(v, k).start()
        t = K1w[...] + Q2w[b].astype(f32)
        K2w[...] = t
        P3w[...] = t.astype(bf)
        for k in (1, 2, 3):
            @pl.when(zx(k) == j)
            def _():
                s3w(v, k).start()

    def out_copies(v):
        l, j = vl(v)
        return [pltpu.make_async_copy(Og.at[g, :, pl.ds(h * HC, HC)], o.at[l, :, pl.ds(pl.multiple_of(h * (FC * 2) + j * HC, 128), HC)],
                                      out_sem.at[g * 2 + h]) for g, o in enumerate((owg, owu)) for h in range(2)]

    def outw(l):
        return pltpu.make_async_copy(Ow.at[l], owd.at[l], outw_sem.at[l])

    def A3(v):
        l, j = vl(v)
        b = v % 2
        for k in (1, 2, 3):
            s3(v, k).wait_recv()

        @pl.when(v > 0)
        def _():
            for d in out_copies(v - 1):
                d.wait()
        Og[...] = (K2g[...] + Q3g[b, 0].astype(f32) + Q3g[b, 1].astype(f32) + Q3g[b, 2].astype(f32)).astype(bf)
        for d in out_copies(v):
            d.start()

        @pl.when(z == j)
        def _():
            for k in (1, 2, 3):
                s3w(v, k).wait_recv()
            Ow[l] = (K2w[...] + Q3w[0].astype(f32) + Q3w[1].astype(f32) + Q3w[2].astype(f32)).astype(bf)
            outw(l).start()

    def rows_of(t, s=0, n=None):
        return pl.ds(t * TM + s * SUB, SUB if n is None else n)

    def weight(l, j, g):
        return G[l, j, g].reshape(D, FC)

    QS = TM // NQ

    def pieces(t, f):
        def body(q, _):
            f(pl.ds(pl.multiple_of(t * TM + q * QS, QS), QS), pl.ds(pl.multiple_of(q * QS, QS), QS))
            return 0
        lax.fori_loop(0, NQ, body, 0)

    def norm_rows(h, r):
        wide = h.astype(f32)
        a = (wide * scale_of(wide)).astype(bf)
        A[r, :] = a
        AT[:, r] = a.T

    def load(src, t, dst, sem):
        return pltpu.make_async_copy(src.at[pl.ds(t * TM, TM)], dst, sem)

    def f0_step(i, t):
        l, j = 0, jmap(i)
        for s in range(2):
            r = rows_of(t, s)
            gate = mm(A[r, :], weight(l, j, 0))
            up = mm(A[r, :], weight(l, j, 1))
            act = (gate * sigmoid(gate) * up).astype(bf)
            act_s[0, s * SUB:(s + 1) * SUB, :] = act
        w = W[l, j].reshape(FC, D)
        for s in range(2):
            r = rows_of(t, s)
            o = mm(act_s[0, s * SUB:(s + 1) * SUB, :], w)
            ACC[r, :] = ACC[r, :] + o

    def fwd(l, j, t):
        b = t % 2
        for s in range(2):
            r = rows_of(t, s)
            rs = slice(s * SUB, (s + 1) * SUB)
            gate = mm(A[r, :], weight(l, j, 0))
            up = mm(A[r, :], weight(l, j, 1))
            dact = mm(DO[r, :], wdt[...]).astype(bf).astype(f32)
            sig = sigmoid(gate)
            silu = gate * sig
            act_s[b, rs, :] = (silu * up).astype(bf)
            dgu[b, rs, FC:] = (dact * silu).astype(bf)
            dgu[b, rs, :FC] = (dact * up * (sig + silu * (1.0 - sig))).astype(bf)

    def bwd(l, j, t):
        b = t % 2
        r = rows_of(t, 0, TM)
        new_g = mm(AT[:, r], dgu[b, :, :FC])
        new_u = mm(AT[:, r], dgu[b, :, FC:])
        new_d = mm(DOT[:, r], act_s[b])
        if t == 0:
            ag[...] = new_g.reshape(ag.shape)
            au[...] = new_u.reshape(au.shape)
            ad[...] = new_d
        else:
            ag[...] += new_g.reshape(ag.shape)
            au[...] += new_u.reshape(au.shape)
            ad[...] += new_d
        for s in range(2):
            r = rows_of(t, s)
            ACC[r, :] += mm(dgu[b, s * SUB:(s + 1) * SUB, :], wt[...])

    for l in range(L):
        for d in own_copies(l):
            d.start()
    for t in range(NT):
        load(x, t, DO.at[pl.ds(t * TM, TM)], tile_sem.at[t]).start()
    for t in range(2):
        load(dy, t, H.at[t], tile2_sem.at[t]).start()
    barrier = pltpu.get_barrier_semaphore()
    peers = [partner, ypeer] + zpeer[1:]
    for dev in peers:
        pl.semaphore_signal(barrier, inc=1, device_id=dev, device_id_type=MESH)
    pl.semaphore_wait(barrier, len(peers))
    for d in own_copies(0):
        d.wait()
    for u in range(NJ):
        R1(u)
    for d in own_copies(1):
        d.wait()
    for t in range(NT):
        load(x, t, DO.at[pl.ds(t * TM, TM)], tile_sem.at[t]).wait()
        load(dy, t, H.at[t % 2], tile2_sem.at[t % 2]).wait()

        def first(r, q):
            norm_rows(DO[r, :], r)
            ACC[r, :] = jnp.zeros_like(ACC[r, :])
            DOT[:, r] = H[t % 2, q, :].T
        pieces(t, first)
        if t + 2 < NT:
            load(dy, t + 2, H.at[t % 2], tile2_sem.at[t % 2]).start()
        if t == 0:
            E(0, 1)
        if t == 1:
            E(0, 2)
        if t == 2:
            E(0, 3)
            Ew(0)
    E(1, 1)
    E(1, 2)
    E4(0)
    E(1, 3)
    Ew(1)

    def f0_chunk(i, _):
        E5(i)
        f0_step(i, 0)

        @pl.when(i < 2)
        def _():
            E(i + 2, 1)
            E(i + 2, 2)

        @pl.when(i == 2)
        def _():
            for u in range(NJ, 2 * NJ):
                R1(u)

        @pl.when(i == 3)
        def _():
            E(NJ, 1)
            E(NJ, 2)
        f0_step(i, 1)
        f0_step(i, 2)

        @pl.when(i < 3)
        def _():
            E4(i + 1)
        f0_step(i, 3)

        @pl.when(i < 2)
        def _():
            E(i + 2, 3)
            Ew(i + 2)

        @pl.when(i == 3)
        def _():
            E(NJ, 3)
            Ew(NJ)
        return 0

    lax.fori_loop(0, NJ, f0_chunk, 0)

    for t in range(NT):
        def second(r, q):
            h = DO[r, :] + ACC[r, :].astype(bf)
            DO[r, :] = h
            ACC[r, :] = jnp.zeros_like(ACC[r, :])
            norm_rows(h, r)
        pieces(t, second)
        pltpu.make_async_copy(DO.at[pl.ds(t * TM, TM)], h1.at[pl.ds(t * TM, TM)], tile_sem.at[t]).start()
    E4(NJ)
    for t in range(NT):
        pltpu.make_async_copy(DO.at[pl.ds(t * TM, TM)], h1.at[pl.ds(t * TM, TM)], tile_sem.at[t]).wait()
        load(dy, t, DO.at[pl.ds(t * TM, TM)], tile_sem.at[t]).start()
    for t in range(NT):
        load(dy, t, DO.at[pl.ds(t * TM, TM)], tile_sem.at[t]).wait()

    def layer_back(n, _):
        l = L - 1 - n

        def chunk(i, _):
            j = jmap(i)
            v = n * NJ + i
            u = NJ + i

            @pl.when(n == 0)
            def _():
                E5(u)
            wt[:FC] = weight(l, j, 0).T
            wt[FC:] = weight(l, j, 1).T
            wdt[...] = W[l, j].reshape(FC, D).T
            fwd(l, j, 0)

            @pl.when(v > 0)
            def _():
                A1S2(v - 1)
            bwd(l, j, 0)
            fwd(l, j, 1)

            @pl.when(v > 1)
            def _():
                A3(v - 2)

            @pl.when((n == 0) & (i < NJ - 1))
            def _():
                E(u + 1, 1)
                E(u + 1, 2)
                E(u + 1, 3)
                Ew(u + 1)
            bwd(l, j, 1)
            fwd(l, j, 2)

            @pl.when(v > 0)
            def _():
                A2S3(v - 1)
            bwd(l, j, 2)
            fwd(l, j, 3)

            @pl.when((n == 0) & (i < NJ - 1))
            def _():
                E4(u + 1)
            bwd(l, j, 3)
            S1(v)
            return 0

        lax.fori_loop(0, NJ, chunk, 0)

        def hload(t):
            return pltpu.make_async_copy(h1.at[pl.ds(t * TM, TM)], H.at[t % 2], tile2_sem.at[t % 2])

        def xload(t):
            return pltpu.make_async_copy(x.at[pl.ds(t * TM, TM)], H.at[t % 2], tile2_sem.at[t % 2])

        def start_h(t):
            @pl.when(n == 0)
            def _():
                hload(t).start()

            @pl.when(n == 1)
            def _():
                xload(t).start()

        start_h(0)
        start_h(1)
        for t in range(NT):
            xload(t).wait()
            def third(r, q):
                wide = H[t % 2, q, :].astype(f32)
                scale = scale_of(wide)
                g = ACC[r, :].astype(bf).astype(f32)
                m = jnp.mean(g * wide, -1, keepdims=True)
                back = (g * scale - wide * (scale * scale * scale * m)).astype(bf)
                o = DO[r, :] + back
                DO[r, :] = o
                ACC[r, :] = jnp.zeros_like(ACC[r, :])
                DOT[:, r] = o.T
            pieces(t, third)
            if t + 2 < NT:
                start_h(t + 2)

            @pl.when(n == 1)
            def _():
                pltpu.make_async_copy(DO.at[pl.ds(t * TM, TM)], dx.at[pl.ds(t * TM, TM)], tile_sem.at[t]).start()

        @pl.when(n == 0)
        def _():
            for t in range(2):
                xload(t).start()
            for t in range(NT):
                xload(t).wait()
                pieces(t, lambda r, q: norm_rows(H[t % 2, q, :], r))
                if t + 2 < NT:
                    xload(t + 2).start()
        return 0

    lax.fori_loop(0, L, layer_back, 0)
    last = L * NJ - 1
    A1S2(last)
    A3(last - 1)
    A2S3(last)
    A3(last)
    for u in range(L * NJ):
        ag_finish(u)
    for d in s1(last) + s2(last):
        d.wait_send()
    s3_sent(last)
    for d in out_copies(last):
        d.wait()
    for l in range(L):
        outw(l).wait()
    for t in range(NT):
        pltpu.make_async_copy(DO.at[pl.ds(t * TM, TM)], dx.at[pl.ds(t * TM, TM)], tile_sem.at[t]).wait()


def solution(mesh):
    def step(x, dy, wg, wu, wd):
        x, dy = x[0], dy[0]
        L, R, FF = wg.shape
        T, D = x.shape
        FR = wd.shape[1]
        FC = NJ * FR
        TM = T // NT
        V, S = pltpu.VMEM, pltpu.SemaphoreType.DMA
        scratch = [
            V((L, NJ, 2, Y, Z, C, R, FC), bf), V((L, NJ, Y, C, FR, D), bf),
            V((T, D), bf), V((D, T), bf), V((T, D), bf), V((D, T), bf), V((T, D), f32),
            V((Y, Z, C, R, FC), f32), V((Y, Z, C, R, FC), f32), V((D, FC), f32),
            V((2, TM, FC), bf), V((2, TM, 2 * FC), bf), V((2 * FC, D), bf), V((D, FC), bf),
            V((2, Y, Z, R, FC), bf), V((Y, FR, D), bf), V((2, 2, Y, Z, R, FC), bf), V((2, Y, FR, D), bf),
            V((2, Z, R, FC), bf), V((FR, D), bf), V((2, 2, Z, R, FC), bf), V((2, FR, D), bf),
            V((2, Z, R, FC), f32), V((FR, D), f32),
            V((4, 2, R, FC), bf), V((FR, D), bf), V((2, R, FC), f32), V((FR, D), f32),
            V((2, 3, 2, R, FC), bf), V((3, FR, D), bf), V((2, R, FC), bf), V((L, FR, D), bf),
            S((L, NJ * 4 + 1)), S((NT,)), S((2,)), S((L * NJ, 13)), S((L * NJ, 11)), S((8,)), S((2, 10)), S((4,)), S((L,)),
        ]
        any_ = pl.BlockSpec(memory_space=pl.ANY)
        dx, g, u, d, _ = pl.pallas_call(
            kernel,
            out_shape=[jax.ShapeDtypeStruct(s, bf) for s in ((T, D), wg.shape, wu.shape, wd.shape, (T, D))],
            in_specs=[any_] * 5,
            out_specs=[any_] * 5,
            scratch_shapes=scratch,
            compiler_params=pltpu.CompilerParams(collective_id=0, has_side_effects=True, vmem_limit_bytes=67043328),
            name="stack",
        )(x, dy, wg, wu, wd)
        return dx[None], g, u, d

    w = P(None, "dp", None)
    t = P(("rep", "dp"), None, None)
    o = P("rep", "dp", None)
    return jax.shard_map(step, mesh=mesh, in_specs=(t, t, w, w, w), out_specs=(t, o, o, o), check_vma=False)
```

```python
import functools

import jax
import jax.numpy as jnp
from jax import lax
from jax.experimental import pallas as pl
from jax.experimental.pallas import tpu as pltpu
from jax.sharding import PartitionSpec as P

MESH = pl.DeviceIdType.MESH
Y, Z, C = 2, 4, 2
NJ = 4
NT = 4
NQ = 4
bf, f32 = jnp.bfloat16, jnp.float32


def mm(a, b):
    return jnp.dot(a, b, preferred_element_type=f32)


def sigmoid(v):
    return 0.5 * jnp.tanh(0.5 * v) + 0.5


def scale_of(wide):
    return lax.rsqrt(jnp.mean(wide * wide, -1, keepdims=True) + 1e-6)


def kernel(x, dy, wg, wu, wd, dx, owg, owu, owd, h1, a0, a0t, G, W, A, AT, DO, DOT, ACC, ag, au, ad, act_s, dgu, wt, wdt,
           P1g, P1w, Q1g, Q1w, P2g, P2w, Q2g, Q2w, K1g, K1w, P3g, P3w, K2g, K2w, Q3g, Q3w, Og, Ow,
           own_sem, tile_sem, tile2_sem, ags, agr, rss, rsr, out_sem, outw_sem, a0_sem):
    L = wg.shape[0]
    T, D = A.shape
    H = act_s
    TM = T // NT
    SUB = TM // 2
    R = wg.shape[1]
    FR = wd.shape[1]
    FC = NJ * FR
    HC = FC // 2
    me = lax.axis_index("dp")
    xi = lax.axis_index("rep")
    xpeer = {"rep": 1 - xi}
    y, z, c = me // (Z * C), (me // C) % Z, me % C

    def dp(yy, zz, cc):
        return {"dp": (yy * Z + zz) * C + cc}

    partner, ypeer = dp(y, z, 1 - c), dp(1 - y, z, c)

    def zx(k):
        hi, lo = z // 2, z % 2
        if k & 2:
            hi = 1 - hi
        if k & 1:
            lo = 1 - lo
        return hi * 2 + lo

    zpeer = [None] + [dp(y, zx(k), c) for k in (1, 2, 3)]
    jmap = lambda i: i + 1 - 2 * (i % 2)

    def remote(src, dst, ss, rs, dev):
        return pltpu.make_async_remote_copy(src_ref=src, dst_ref=dst, send_sem=ss, recv_sem=rs, device_id=dev, device_id_type=MESH)

    def li(u):
        return u // NJ, jmap(u % NJ)

    def own_copies(l):
        out = []
        for j in range(NJ):
            for g, w in enumerate((wg, wu)):
                for h in range(2):
                    out.append(pltpu.make_async_copy(
                        w.at[l, :, pl.ds(h * (FC * 2) + j * HC, HC)], G.at[l, j, g, y, z, c, :, pl.ds(h * HC, HC)],
                        own_sem.at[l, (j * 2 + g) * 2 + h]))
        out.append(pltpu.make_async_copy(wd.at[l], W.at[l, z, y, c], own_sem.at[l, NJ * 4]))
        return out

    def g_ref(u, yy, zz, xx=None):
        l, j = li(u)
        return G.at[l, j, xi if xx is None else xx, yy, zz, c]

    def w_ref(u, yy, xx=None):
        l, j = li(u)
        return W.at[l, j, yy, c, pl.ds(pl.multiple_of((xi if xx is None else xx) * (FR // 2), FR // 2), FR // 2)]

    def same(ref, u, ss, rs, dev):
        return remote(ref, ref, ags.at[u, ss], agr.at[u, rs], dev)

    def ag_z(u, k, zz):
        return same(g_ref(u, y, zz), u, k - 1, k - 1, zpeer[k])

    def ag_zw(u, k):
        return same(w_ref(u, y), u, 2 + k, 3, zpeer[k])

    def ag_y(u, k, yy):
        return same(g_ref(u, yy, zx(k)), u, 6 + k, 4 + k, ypeer)

    def ag_yw(u, yy):
        return same(w_ref(u, yy), u, 10, 8, ypeer)

    def ag_x(u, k, xx=None):
        return same(g_ref(u, y, zx(k), xx), u, 12 + k, 10 + k, xpeer)

    def ag_xy(u, k, xx=None):
        return same(g_ref(u, 1 - y, zx(k), xx), u, 16 + k, 14 + k, xpeer)

    def ag_xw(u, xx=None):
        return same(w_ref(u, y, xx), u, 20, 18, xpeer)

    def ag_xyw(u, xx=None):
        return same(w_ref(u, 1 - y, xx), u, 21, 19, xpeer)

    def ag_p(u, cc):
        l, j = li(u)
        ref = G.at[l, j, :, :, :, cc]
        return remote(ref, ref, ags.at[u, 11], agr.at[u, 9], partner)

    def ag_pw(u, cc):
        l, j = li(u)
        ref = W.at[l, j, :, cc]
        return remote(ref, ref, ags.at[u, 12], agr.at[u, 10], partner)

    def R1(u):
        l, j = li(u)
        for k in (1, 2, 3):
            ag_z(u, k, z).start()
        ag_y(u, 0, y).start()

        @pl.when(z == j)
        def _():
            for k in (1, 2, 3):
                ag_zw(u, k).start()
            ag_yw(u, y).start()

    def E(u):
        l, j = li(u)
        for k in (1, 2, 3):
            ag_z(u, k, zx(k)).wait_recv()
            ag_y(u, k, y).start()
            ag_x(u, k).start()
            if k == 1:
                ag_y(u, 0, 1 - y).wait_recv()
                ag_xy(u, 0).start()

        @pl.when(z != j)
        def _():
            ag_zw(u, 1).wait_recv()
            ag_yw(u, y).start()
            ag_xw(u).start()

    def E4(u):
        for k in (1, 2, 3):
            ag_y(u, k, 1 - y).wait_recv()
            ag_xy(u, k).start()
        ag_yw(u, 1 - y).wait_recv()
        ag_xyw(u).start()

    def Ex(u):
        l, j = li(u)
        for k in (1, 2, 3):
            ag_x(u, k, 1 - xi).wait_recv()
        for k in range(4):
            ag_xy(u, k, 1 - xi).wait_recv()
        ag_xyw(u, 1 - xi).wait_recv()

        @pl.when(z != j)
        def _():
            ag_xw(u, 1 - xi).wait_recv()
        ag_p(u, c).start()
        ag_pw(u, c).start()

    def E5(u):
        ag_p(u, 1 - c).wait_recv()
        ag_pw(u, 1 - c).wait_recv()

    def ag_finish(u):
        l, j = li(u)
        for k in (1, 2, 3):
            ag_z(u, k, z).wait_send()
            ag_x(u, k).wait_send()
        for k in range(4):
            ag_y(u, k, y).wait_send()

        @pl.when(z == j)
        def _():
            for k in (1, 2, 3):
                ag_zw(u, k).wait_send()

        @pl.when(z != j)
        def _():
            ag_xw(u).wait_send()
        ag_yw(u, y).wait_send()
        for k in range(4):
            ag_xy(u, k).wait_send()
        ag_xyw(u).wait_send()
        ag_p(u, c).wait_send()
        ag_pw(u, c).wait_send()

    def vl(v):
        return L - 1 - v // NJ, jmap(v % NJ)

    def s1(v):
        b = v % 2
        return (remote(P1g, Q1g.at[b], rss.at[0], rsr.at[b, 0], partner), remote(P1w, Q1w.at[b], rss.at[1], rsr.at[b, 1], partner))

    def s2(v):
        b = v % 2
        return (remote(P2g, Q2g.at[b], rss.at[2], rsr.at[b, 2], ypeer), remote(P2w, Q2w.at[b], rss.at[3], rsr.at[b, 3], ypeer))

    def s3(v, k):
        b = v % 2
        return remote(P3g.at[k], Q3g.at[b, k - 1], rss.at[3 + k], rsr.at[b, 3 + k], zpeer[k])

    def s3w(v, k):
        b = v % 2
        return remote(P3w, Q3w.at[k - 1], rss.at[7], rsr.at[b, 6 + k], zpeer[k])

    def wrows(yy, cc):
        return pl.ds(pl.multiple_of((yy * C + cc) * FR, FR), FR)

    def S1(v):
        @pl.when(v > 0)
        def _():
            for d in s1(v - 1):
                d.wait_send()
        for g, acc in enumerate((ag, au)):
            P1g[g] = acc[:, :, 1 - c].astype(bf)
        ad[...] = ad[...].T
        for yy in range(Y):
            P1w[yy] = ad[wrows(yy, 1 - c), :].astype(bf)
        for d in s1(v):
            d.start()

    def A1S2(v):
        b = v % 2
        for d in s1(v):
            d.wait_recv()

        @pl.when(v > 0)
        def _():
            for d in s2(v - 1):
                d.wait_send()
        for g, acc in enumerate((ag, au)):
            K1g[g] = acc[y, :, c] + Q1g[b, g, y].astype(f32)
            P2g[g] = (acc[1 - y, :, c] + Q1g[b, g, 1 - y].astype(f32)).astype(bf)
        K1w[...] = ad[wrows(y, c), :] + Q1w[b, y].astype(f32)
        P2w[...] = (ad[wrows(1 - y, c), :] + Q1w[b, 1 - y].astype(f32)).astype(bf)
        for d in s2(v):
            d.start()

    def s3_sent(v):
        l, j = vl(v)
        for k in (1, 2, 3):
            s3(v, k).wait_send()

        @pl.when(z != j)
        def _():
            s3w(v, 1).wait_send()

    def A2S3(v):
        l, j = vl(v)
        b = v % 2
        s2(v)[0].wait_recv()

        @pl.when(v > 0)
        def _():
            s3_sent(v - 1)
        for k in range(4):
            t = K1g[:, zx(k)] + Q2g[b, :, zx(k)].astype(f32)
            if k == 0:
                K2g[...] = t
            else:
                P3g[k] = t.astype(bf)
                s3(v, k).start()
        s2(v)[1].wait_recv()
        t = K1w[...] + Q2w[b].astype(f32)
        K2w[...] = t
        P3w[...] = t.astype(bf)
        for k in (1, 2, 3):
            @pl.when(zx(k) == j)
            def _():
                s3w(v, k).start()

    def out_copies(v):
        l, j = vl(v)
        return [pltpu.make_async_copy(Og.at[g, :, pl.ds(h * HC, HC)], o.at[l, :, pl.ds(pl.multiple_of(h * (FC * 2) + j * HC, 128), HC)],
                                      out_sem.at[g * 2 + h]) for g, o in enumerate((owg, owu)) for h in range(2)]

    def outw(l):
        return pltpu.make_async_copy(Ow.at[l], owd.at[l], outw_sem.at[l])

    def A3(v):
        l, j = vl(v)
        b = v % 2
        for k in (1, 2, 3):
            s3(v, k).wait_recv()

        @pl.when(v > 0)
        def _():
            for d in out_copies(v - 1):
                d.wait()
        Og[...] = (K2g[...] + Q3g[b, 0].astype(f32) + Q3g[b, 1].astype(f32) + Q3g[b, 2].astype(f32)).astype(bf)
        for d in out_copies(v):
            d.start()

        @pl.when(z == j)
        def _():
            for k in (1, 2, 3):
                s3w(v, k).wait_recv()
            Ow[l] = (K2w[...] + Q3w[0].astype(f32) + Q3w[1].astype(f32) + Q3w[2].astype(f32)).astype(bf)
            outw(l).start()

    def rows_of(t, s=0, n=None):
        return pl.ds(t * TM + s * SUB, SUB if n is None else n)

    def weight(l, j, g):
        return G[l, j, g].reshape(D, FC)

    QS = TM // NQ

    def pieces(t, f):
        def body(q, _):
            f(pl.ds(pl.multiple_of(t * TM + q * QS, QS), QS), pl.ds(pl.multiple_of(q * QS, QS), QS))
            return 0
        lax.fori_loop(0, NQ, body, 0)

    def norm_rows(h, r):
        wide = h.astype(f32)
        a = (wide * scale_of(wide)).astype(bf)
        A[r, :] = a
        AT[:, r] = a.T

    def load(src, t, dst, sem):
        return pltpu.make_async_copy(src.at[pl.ds(t * TM, TM)], dst, sem)

    def a0_out():
        return [pltpu.make_async_copy(A, a0, a0_sem.at[0]), pltpu.make_async_copy(AT, a0t, a0_sem.at[1])]

    def a0_in():
        return [pltpu.make_async_copy(a0, A, a0_sem.at[0]), pltpu.make_async_copy(a0t, AT, a0_sem.at[1])]

    def f0_step(i, t):
        l, j = 0, jmap(i)
        for s in range(2):
            r = rows_of(t, s)
            gate = mm(A[r, :], weight(l, j, 0))
            up = mm(A[r, :], weight(l, j, 1))
            act = (gate * sigmoid(gate) * up).astype(bf)
            act_s[0, s * SUB:(s + 1) * SUB, :] = act
        w = W[l, j].reshape(FC, D)
        for s in range(2):
            r = rows_of(t, s)
            o = mm(act_s[0, s * SUB:(s + 1) * SUB, :], w)
            ACC[r, :] = ACC[r, :] + o

    def fwd(l, j, t):
        b = t % 2
        for s in range(2):
            r = rows_of(t, s)
            rs = slice(s * SUB, (s + 1) * SUB)
            gate = mm(A[r, :], weight(l, j, 0))
            up = mm(A[r, :], weight(l, j, 1))
            dact = mm(DO[r, :], wdt[...]).astype(bf).astype(f32)
            sig = sigmoid(gate)
            silu = gate * sig
            act_s[b, rs, :] = (silu * up).astype(bf)
            dgu[b, rs, FC:] = (dact * silu).astype(bf)
            dgu[b, rs, :FC] = (dact * up * (sig + silu * (1.0 - sig))).astype(bf)

    def bwd(l, j, t):
        b = t % 2
        r = rows_of(t, 0, TM)
        new_g = mm(AT[:, r], dgu[b, :, :FC])
        new_u = mm(AT[:, r], dgu[b, :, FC:])
        new_d = mm(DOT[:, r], act_s[b])
        if t == 0:
            ag[...] = new_g.reshape(ag.shape)
            au[...] = new_u.reshape(au.shape)
            ad[...] = new_d
        else:
            ag[...] += new_g.reshape(ag.shape)
            au[...] += new_u.reshape(au.shape)
            ad[...] += new_d
        if t < NT - 1:
            bwd_a(t)

    def bwd_a(t):
        for s in range(2):
            r = rows_of(t, s)
            ACC[r, :] += mm(dgu[t % 2, s * SUB:(s + 1) * SUB, :], wt[...])

    for l in range(L):
        for d in own_copies(l):
            d.start()
    for t in range(NT):
        load(x, t, DO.at[pl.ds(t * TM, TM)], tile_sem.at[t]).start()
    for t in range(2):
        load(dy, t, H.at[t], tile2_sem.at[t]).start()
    barrier = pltpu.get_barrier_semaphore()
    peers = [partner, ypeer, xpeer] + zpeer[1:]
    for dev in peers:
        pl.semaphore_signal(barrier, inc=1, device_id=dev, device_id_type=MESH)
    pl.semaphore_wait(barrier, len(peers))
    for d in own_copies(0):
        d.wait()
    R1(0)
    for d in own_copies(1):
        d.wait()
    for t in range(NT):
        load(x, t, DO.at[pl.ds(t * TM, TM)], tile_sem.at[t]).wait()
        load(dy, t, H.at[t % 2], tile2_sem.at[t % 2]).wait()

        def first(r, q):
            norm_rows(DO[r, :], r)
            ACC[r, :] = jnp.zeros_like(ACC[r, :])
            DOT[:, r] = H[t % 2, q, :].T
        pieces(t, first)
        if t + 2 < NT:
            load(dy, t + 2, H.at[t % 2], tile2_sem.at[t % 2]).start()
        if t == 0:
            R1(1)
        if t == 1:
            E(0)
            R1(2)
        if t == 3:
            E4(0)
    for d in a0_out():
        d.start()
    E(1)
    Ex(0)
    E4(1)

    def f0_chunk(i, _):
        E5(i)
        f0_step(i, 0)
        E(i + 2)
        R1(i + 3)
        f0_step(i, 1)
        f0_step(i, 2)
        Ex(i + 1)
        f0_step(i, 3)
        E4(i + 2)
        return 0

    lax.fori_loop(0, NJ, f0_chunk, 0)
    for d in a0_out():
        d.wait()

    for t in range(NT):
        def second(r, q):
            h = DO[r, :] + ACC[r, :].astype(bf)
            DO[r, :] = h
            ACC[r, :] = jnp.zeros_like(ACC[r, :])
            norm_rows(h, r)
        pieces(t, second)
        pltpu.make_async_copy(DO.at[pl.ds(t * TM, TM)], h1.at[pl.ds(t * TM, TM)], tile_sem.at[t]).start()
    for t in range(NT):
        pltpu.make_async_copy(DO.at[pl.ds(t * TM, TM)], h1.at[pl.ds(t * TM, TM)], tile_sem.at[t]).wait()
        load(dy, t, DO.at[pl.ds(t * TM, TM)], tile_sem.at[t]).start()
    for t in range(NT):
        load(dy, t, DO.at[pl.ds(t * TM, TM)], tile_sem.at[t]).wait()

    def layer_back(n, _):
        l = L - 1 - n

        def chunk(i, _):
            j = jmap(i)
            v = n * NJ + i
            u = NJ + i

            @pl.when(n == 0)
            def _():
                E5(u)
            wt[:FC] = weight(l, j, 0).T
            wt[FC:] = weight(l, j, 1).T
            wdt[...] = W[l, j].reshape(FC, D).T
            fwd(l, j, 0)

            @pl.when(i > 0)
            def _():
                A1S2(v - 1)
            bwd(l, j, 0)
            fwd(l, j, 1)

            @pl.when(v > 1)
            def _():
                A3(v - 2)

            @pl.when((n == 0) & (i == 0))
            def _():
                R1(2 * NJ - 1)

            @pl.when((n == 0) & (i < NJ - 2))
            def _():
                E(u + 2)
            bwd(l, j, 1)
            fwd(l, j, 2)

            @pl.when(v > 0)
            def _():
                A2S3(v - 1)
            bwd(l, j, 2)
            fwd(l, j, 3)

            @pl.when((n == 0) & (i < NJ - 2))
            def _():
                E4(u + 2)

            @pl.when((n == 0) & (i < NJ - 1))
            def _():
                Ex(u + 1)
            bwd(l, j, 3)
            S1(v)
            bwd_a(3)
            return 0

        lax.fori_loop(0, NJ, chunk, 0)

        def hload(t):
            return pltpu.make_async_copy(h1.at[pl.ds(t * TM, TM)], H.at[t % 2], tile2_sem.at[t % 2])

        def xload(t):
            return pltpu.make_async_copy(x.at[pl.ds(t * TM, TM)], H.at[t % 2], tile2_sem.at[t % 2])

        def start_h(t):
            @pl.when(n == 0)
            def _():
                hload(t).start()

            @pl.when(n == 1)
            def _():
                xload(t).start()

        start_h(0)
        start_h(1)

        @pl.when(n == 0)
        def _():
            for d in a0_in():
                d.start()
        for t in range(NT):
            xload(t).wait()
            def third(r, q):
                wide = H[t % 2, q, :].astype(f32)
                scale = scale_of(wide)
                g = ACC[r, :].astype(bf).astype(f32)
                m = jnp.mean(g * wide, -1, keepdims=True)
                back = (g * scale - wide * (scale * scale * scale * m)).astype(bf)
                o = DO[r, :] + back
                DO[r, :] = o
                ACC[r, :] = jnp.zeros_like(ACC[r, :])
                DOT[:, r] = o.T
            pieces(t, third)
            if t == 0:
                A1S2(n * NJ + NJ - 1)
            if t + 2 < NT:
                start_h(t + 2)

            @pl.when(n == 1)
            def _():
                pltpu.make_async_copy(DO.at[pl.ds(t * TM, TM)], dx.at[pl.ds(t * TM, TM)], tile_sem.at[t]).start()

        @pl.when(n == 0)
        def _():
            for d in a0_in():
                d.wait()
        return 0

    lax.fori_loop(0, L, layer_back, 0)
    last = L * NJ - 1
    A3(last - 1)
    A2S3(last)
    A3(last)
    for u in range(L * NJ):
        ag_finish(u)
    for d in s1(last) + s2(last):
        d.wait_send()
    s3_sent(last)
    for d in out_copies(last):
        d.wait()
    for l in range(L):
        outw(l).wait()
    for t in range(NT):
        pltpu.make_async_copy(DO.at[pl.ds(t * TM, TM)], dx.at[pl.ds(t * TM, TM)], tile_sem.at[t]).wait()


def hand_over(tiles, rows, *refs):
    src, dst, via, sem = refs[:4], refs[4:8], refs[8:12], refs[12]

    def part(ref, k, t):
        return ref[k].at[pl.ds(t * rows, rows)] if k == 0 else ref[k].at[t]

    into = [pltpu.make_async_copy(part(src, k, t), part(via, k, t), sem.at[n]) for n, (k, t) in enumerate(tiles)]
    out = [pltpu.make_async_copy(part(via, k, t), part(dst, k, t), sem.at[n]) for n, (k, t) in enumerate(tiles)]
    for d in into:
        d.start()
    for a, b in zip(into, out):
        a.wait()
        b.start()
    for d in out:
        d.wait()


def solution(mesh):
    def step(x, dy, wg, wu, wd):
        x, dy = x[0], dy[0]
        L, R, FF = wg.shape
        T, D = x.shape
        FR = wd.shape[1]
        FC = NJ * FR
        TM = T // NT
        V, S = pltpu.VMEM, pltpu.SemaphoreType.DMA
        scratch = [
            V((L, NJ, 2, Y, Z, C, R, FC), bf), V((L, NJ, Y, C, FR, D), bf),
            V((T, D), bf), V((D, T), bf), V((T, D), bf), V((D, T), bf), V((T, D), f32),
            V((Y, Z, C, R, FC), f32), V((Y, Z, C, R, FC), f32), V((D, FC), f32),
            V((2, TM, FC), bf), V((2, TM, 2 * FC), bf), V((2 * FC, D), bf), V((D, FC), bf),
            V((2, Y, Z, R, FC), bf), V((Y, FR, D), bf), V((2, 2, Y, Z, R, FC), bf), V((2, Y, FR, D), bf),
            V((2, Z, R, FC), bf), V((FR, D), bf), V((2, 2, Z, R, FC), bf), V((2, FR, D), bf),
            V((2, Z, R, FC), f32), V((FR, D), f32),
            V((4, 2, R, FC), bf), V((FR, D), bf), V((2, R, FC), f32), V((FR, D), f32),
            V((2, 3, 2, R, FC), bf), V((3, FR, D), bf), V((2, R, FC), bf), V((L, FR, D), bf),
            S((L, NJ * 4 + 1)), S((NT,)), S((2,)), S((L * NJ, 22)), S((L * NJ, 20)), S((8,)), S((2, 10)), S((4,)), S((L,)), S((2,)),
        ]
        any_ = pl.BlockSpec(memory_space=pl.ANY)
        dx, g, u, d, *_ = pl.pallas_call(
            kernel,
            out_shape=[jax.ShapeDtypeStruct(s, bf) for s in ((T, D), wg.shape, wu.shape, wd.shape, (T, D), (T, D), (D, T))],
            in_specs=[any_] * 5,
            out_specs=[any_] * 7,
            scratch_shapes=scratch,
            compiler_params=pltpu.CompilerParams(collective_id=0, has_side_effects=True, vmem_limit_bytes=67043328),
            name="stack",
        )(x, dy, wg, wu, wd)
        outs = (dx, g, u, d)
        tiles = [(k, t) for k in (1, 2, 3) for t in range(L)] + [(0, t) for t in range(8)]
        dx, g, u, d = pl.pallas_call(
            functools.partial(hand_over, tiles, T // 8),
            out_shape=[jax.ShapeDtypeStruct(t.shape, bf) for t in outs],
            in_specs=[any_] * 4,
            out_specs=[any_] * 4,
            scratch_shapes=[V(t.shape, bf) for t in outs] + [S((len(tiles),))],
            compiler_params=pltpu.CompilerParams(vmem_limit_bytes=67043328),
            cost_estimate=pl.CostEstimate(flops=0, bytes_accessed=10 * 2**20, transcendentals=0),
            name="hand_over",
        )(*outs)
        return dx[None], g, u, d

    w = P(None, "dp", None)
    t = P(("rep", "dp"), None, None)
    o = P("rep", "dp", None)
    return jax.shard_map(step, mesh=mesh, in_specs=(t, t, w, w, w), out_specs=(t, o, o, o), check_vma=False)
```

```python
import functools

import jax
import jax.numpy as jnp
from jax import lax
from jax.experimental import pallas as pl
from jax.experimental.pallas import tpu as pltpu
from jax.sharding import PartitionSpec as P

MESH = pl.DeviceIdType.MESH
Y, Z, C = 2, 4, 2
NJ = 4
NT = 4
NQ = 4
bf, f32 = jnp.bfloat16, jnp.float32


def mm(a, b):
    return jnp.dot(a, b, preferred_element_type=f32)


def sigmoid(v):
    return 0.5 * jnp.tanh(0.5 * v) + 0.5


def scale_of(wide):
    return lax.rsqrt(jnp.mean(wide * wide, -1, keepdims=True) + 1e-6)


def kernel(x, dy, wg, wu, wd, dx, owg, owu, owd, h1, a0, a0t, G, W, A, AT, DO, DOT, ACC, ag, au, ad, act_s, dgu, wt, wdt,
           P1g, P1w, Q1g, Q1w, P2g, P2w, Q2g, Q2w, K1g, K1w, P3g, P3w, K2g, K2w, Q3g, Q3w, Og, Ow,
           own_sem, tile_sem, tile2_sem, ags, agr, rss, rsr, out_sem, outw_sem, a0_sem):
    L = wg.shape[0]
    T, D = A.shape
    H = act_s
    TM = T // NT
    SUB = TM // 2
    R = wg.shape[1]
    FR = wd.shape[1]
    FC = NJ * FR
    HC = FC // 2
    me = lax.axis_index("dp")
    xi = lax.axis_index("rep")
    xpeer = {"rep": 1 - xi}
    y, z, c = me // (Z * C), (me // C) % Z, me % C

    def dp(yy, zz, cc):
        return {"dp": (yy * Z + zz) * C + cc}

    partner, ypeer = dp(y, z, 1 - c), dp(1 - y, z, c)

    def zx(k):
        hi, lo = z // 2, z % 2
        if k & 2:
            hi = 1 - hi
        if k & 1:
            lo = 1 - lo
        return hi * 2 + lo

    zpeer = [None] + [dp(y, zx(k), c) for k in (1, 2, 3)]
    jmap = lambda i: i + 1 - 2 * (i % 2)

    def remote(src, dst, ss, rs, dev):
        return pltpu.make_async_remote_copy(src_ref=src, dst_ref=dst, send_sem=ss, recv_sem=rs, device_id=dev, device_id_type=MESH)

    def li(u):
        return u // NJ, jmap(u % NJ)

    def own_copies(l):
        out = []
        for j in range(NJ):
            for g, w in enumerate((wg, wu)):
                for h in range(2):
                    out.append(pltpu.make_async_copy(
                        w.at[l, :, pl.ds(h * (FC * 2) + j * HC, HC)], G.at[l, j, g, y, z, c, :, pl.ds(h * HC, HC)],
                        own_sem.at[l, (j * 2 + g) * 2 + h]))
        out.append(pltpu.make_async_copy(wd.at[l], W.at[l, z, y, c], own_sem.at[l, NJ * 4]))
        return out

    def g_ref(u, yy, zz, xx=None):
        l, j = li(u)
        return G.at[l, j, xi if xx is None else xx, yy, zz, c]

    def w_ref(u, yy, xx=None):
        l, j = li(u)
        return W.at[l, j, yy, c, pl.ds(pl.multiple_of((xi if xx is None else xx) * (FR // 2), FR // 2), FR // 2)]

    def same(ref, u, ss, rs, dev):
        return remote(ref, ref, ags.at[u, ss], agr.at[u, rs], dev)

    def ag_z(u, k, zz):
        return same(g_ref(u, y, zz), u, k - 1, k - 1, zpeer[k])

    def ag_zw(u, k):
        return same(w_ref(u, y), u, 2 + k, 3, zpeer[k])

    def ag_y(u, k, yy):
        return same(g_ref(u, yy, zx(k)), u, 6 + k, 4 + k, ypeer)

    def ag_yw(u, yy):
        return same(w_ref(u, yy), u, 10, 8, ypeer)

    def ag_x(u, k, xx=None):
        return same(g_ref(u, y, zx(k), xx), u, 12 + k, 10 + k, xpeer)

    def ag_xy(u, k, xx=None):
        return same(g_ref(u, 1 - y, zx(k), xx), u, 16 + k, 14 + k, xpeer)

    def ag_xw(u, xx=None):
        return same(w_ref(u, y, xx), u, 20, 18, xpeer)

    def ag_xyw(u, xx=None):
        return same(w_ref(u, 1 - y, xx), u, 21, 19, xpeer)

    def ag_p(u, cc):
        l, j = li(u)
        ref = G.at[l, j, :, :, :, cc]
        return remote(ref, ref, ags.at[u, 11], agr.at[u, 9], partner)

    def ag_pw(u, cc):
        l, j = li(u)
        ref = W.at[l, j, :, cc]
        return remote(ref, ref, ags.at[u, 12], agr.at[u, 10], partner)

    def R1(u):
        l, j = li(u)
        for k in (1, 2, 3):
            ag_z(u, k, z).start()
        ag_y(u, 0, y).start()

        @pl.when(z == j)
        def _():
            for k in (1, 2, 3):
                ag_zw(u, k).start()
            ag_yw(u, y).start()

    def E(u):
        l, j = li(u)
        for k in (1, 2, 3):
            ag_z(u, k, zx(k)).wait_recv()
            ag_y(u, k, y).start()
            ag_x(u, k).start()
            if k == 1:
                ag_y(u, 0, 1 - y).wait_recv()
                ag_xy(u, 0).start()

        @pl.when(z != j)
        def _():
            ag_zw(u, 1).wait_recv()
            ag_yw(u, y).start()
            ag_xw(u).start()

    def E4(u):
        for k in (1, 2, 3):
            ag_y(u, k, 1 - y).wait_recv()
            ag_xy(u, k).start()
        ag_yw(u, 1 - y).wait_recv()
        ag_xyw(u).start()

    def Ex(u):
        l, j = li(u)
        for k in (1, 2, 3):
            ag_x(u, k, 1 - xi).wait_recv()
        for k in range(4):
            ag_xy(u, k, 1 - xi).wait_recv()
        ag_xyw(u, 1 - xi).wait_recv()

        @pl.when(z != j)
        def _():
            ag_xw(u, 1 - xi).wait_recv()
        ag_p(u, c).start()
        ag_pw(u, c).start()

    def E5(u):
        ag_p(u, 1 - c).wait_recv()
        ag_pw(u, 1 - c).wait_recv()

    def ag_finish(u):
        l, j = li(u)
        for k in (1, 2, 3):
            ag_z(u, k, z).wait_send()
            ag_x(u, k).wait_send()
        for k in range(4):
            ag_y(u, k, y).wait_send()

        @pl.when(z == j)
        def _():
            for k in (1, 2, 3):
                ag_zw(u, k).wait_send()

        @pl.when(z != j)
        def _():
            ag_xw(u).wait_send()
        ag_yw(u, y).wait_send()
        for k in range(4):
            ag_xy(u, k).wait_send()
        ag_xyw(u).wait_send()
        ag_p(u, c).wait_send()
        ag_pw(u, c).wait_send()

    def vl(v):
        return L - 1 - v // NJ, jmap(v % NJ)

    def s1(v):
        b = v % 2
        return (remote(P1g, Q1g.at[b], rss.at[0], rsr.at[b, 0], partner), remote(P1w, Q1w.at[b], rss.at[1], rsr.at[b, 1], partner))

    def s2(v):
        b = v % 2
        return (remote(P2g, Q2g.at[b], rss.at[2], rsr.at[b, 2], ypeer), remote(P2w, Q2w.at[b], rss.at[3], rsr.at[b, 3], ypeer))

    def s3(v, k):
        b = v % 2
        return remote(P3g.at[k], Q3g.at[b, k - 1], rss.at[3 + k], rsr.at[b, 3 + k], zpeer[k])

    def s3w(v, k):
        b = v % 2
        return remote(P3w, Q3w.at[k - 1], rss.at[7], rsr.at[b, 6 + k], zpeer[k])

    def wrows(yy, cc):
        return pl.ds(pl.multiple_of((yy * C + cc) * FR, FR), FR)

    def S1(v):
        @pl.when(v > 0)
        def _():
            for d in s1(v - 1):
                d.wait_send()
        for g, acc in enumerate((ag, au)):
            P1g[g] = acc[:, :, 1 - c].astype(bf)
        ad[...] = ad[...].T
        for yy in range(Y):
            P1w[yy] = ad[wrows(yy, 1 - c), :].astype(bf)
        for d in s1(v):
            d.start()

    def A1S2(v):
        b = v % 2
        for d in s1(v):
            d.wait_recv()

        @pl.when(v > 0)
        def _():
            for d in s2(v - 1):
                d.wait_send()
        for g, acc in enumerate((ag, au)):
            K1g[g] = acc[y, :, c] + Q1g[b, g, y].astype(f32)
            P2g[g] = (acc[1 - y, :, c] + Q1g[b, g, 1 - y].astype(f32)).astype(bf)
        K1w[...] = ad[wrows(y, c), :] + Q1w[b, y].astype(f32)
        P2w[...] = (ad[wrows(1 - y, c), :] + Q1w[b, 1 - y].astype(f32)).astype(bf)
        for d in s2(v):
            d.start()

    def s3_sent(v):
        l, j = vl(v)
        for k in (1, 2, 3):
            s3(v, k).wait_send()

        @pl.when(z != j)
        def _():
            s3w(v, 1).wait_send()

    def A2S3(v):
        l, j = vl(v)
        b = v % 2
        s2(v)[0].wait_recv()

        @pl.when(v > 0)
        def _():
            s3_sent(v - 1)
        for k in range(4):
            t = K1g[:, zx(k)] + Q2g[b, :, zx(k)].astype(f32)
            if k == 0:
                K2g[...] = t
            else:
                P3g[k] = t.astype(bf)
                s3(v, k).start()
        s2(v)[1].wait_recv()
        t = K1w[...] + Q2w[b].astype(f32)
        K2w[...] = t
        P3w[...] = t.astype(bf)
        for k in (1, 2, 3):
            @pl.when(zx(k) == j)
            def _():
                s3w(v, k).start()

    def out_copies(v):
        l, j = vl(v)
        return [pltpu.make_async_copy(Og.at[g, :, pl.ds(h * HC, HC)], o.at[l, :, pl.ds(pl.multiple_of(h * (FC * 2) + j * HC, 128), HC)],
                                      out_sem.at[g * 2 + h]) for g, o in enumerate((owg, owu)) for h in range(2)]

    def outw(l):
        return pltpu.make_async_copy(Ow.at[l], owd.at[l], outw_sem.at[l])

    def A3(v):
        l, j = vl(v)
        b = v % 2
        for k in (1, 2, 3):
            s3(v, k).wait_recv()

        @pl.when(v > 0)
        def _():
            for d in out_copies(v - 1):
                d.wait()
        Og[...] = (K2g[...] + Q3g[b, 0].astype(f32) + Q3g[b, 1].astype(f32) + Q3g[b, 2].astype(f32)).astype(bf)
        for d in out_copies(v):
            d.start()

        @pl.when(z == j)
        def _():
            for k in (1, 2, 3):
                s3w(v, k).wait_recv()
            Ow[l] = (K2w[...] + Q3w[0].astype(f32) + Q3w[1].astype(f32) + Q3w[2].astype(f32)).astype(bf)
            outw(l).start()

    def rows_of(t, s=0, n=None):
        return pl.ds(t * TM + s * SUB, SUB if n is None else n)

    def weight(l, j, g):
        return G[l, j, g].reshape(D, FC)

    QS = TM // NQ

    def pieces(t, f):
        def body(q, _):
            f(pl.ds(pl.multiple_of(t * TM + q * QS, QS), QS), pl.ds(pl.multiple_of(q * QS, QS), QS))
            return 0
        lax.fori_loop(0, NQ, body, 0)

    def norm_rows(h, r):
        wide = h.astype(f32)
        a = (wide * scale_of(wide)).astype(bf)
        A[r, :] = a
        AT[:, r] = a.T

    def load(src, t, dst, sem):
        return pltpu.make_async_copy(src.at[pl.ds(t * TM, TM)], dst, sem)

    def a0_out():
        return [pltpu.make_async_copy(A, a0, a0_sem.at[0]), pltpu.make_async_copy(AT, a0t, a0_sem.at[1])]

    def a0_in():
        return [pltpu.make_async_copy(a0, A, a0_sem.at[0]), pltpu.make_async_copy(a0t, AT, a0_sem.at[1])]

    def f0_step(i, t):
        l, j = 0, jmap(i)
        for s in range(2):
            r = rows_of(t, s)
            gate = mm(A[r, :], weight(l, j, 0))
            up = mm(A[r, :], weight(l, j, 1))
            act = (gate * sigmoid(gate) * up).astype(bf)
            act_s[0, s * SUB:(s + 1) * SUB, :] = act
        w = W[l, j].reshape(FC, D)
        for s in range(2):
            r = rows_of(t, s)
            o = mm(act_s[0, s * SUB:(s + 1) * SUB, :], w)
            ACC[r, :] = ACC[r, :] + o

    def fwd(l, j, t):
        b = t % 2
        for s in range(2):
            r = rows_of(t, s)
            rs = slice(s * SUB, (s + 1) * SUB)
            gate = mm(A[r, :], weight(l, j, 0))
            up = mm(A[r, :], weight(l, j, 1))
            dact = mm(DO[r, :], wdt[...]).astype(bf).astype(f32)
            sig = sigmoid(gate)
            silu = gate * sig
            act_s[b, rs, :] = (silu * up).astype(bf)
            dgu[b, rs, FC:] = (dact * silu).astype(bf)
            dgu[b, rs, :FC] = (dact * up * (sig + silu * (1.0 - sig))).astype(bf)

    def bwd(l, j, t):
        b = t % 2
        r = rows_of(t, 0, TM)
        new_g = mm(AT[:, r], dgu[b, :, :FC])
        new_u = mm(AT[:, r], dgu[b, :, FC:])
        new_d = mm(DOT[:, r], act_s[b])
        if t == 0:
            ag[...] = new_g.reshape(ag.shape)
            au[...] = new_u.reshape(au.shape)
            ad[...] = new_d
        else:
            ag[...] += new_g.reshape(ag.shape)
            au[...] += new_u.reshape(au.shape)
            ad[...] += new_d
        if t < NT - 1:
            bwd_a(t)

    def bwd_a(t):
        for s in range(2):
            r = rows_of(t, s)
            ACC[r, :] += mm(dgu[t % 2, s * SUB:(s + 1) * SUB, :], wt[...])

    for l in range(L):
        for d in own_copies(l):
            d.start()
    for t in range(NT):
        load(x, t, DO.at[pl.ds(t * TM, TM)], tile_sem.at[t]).start()
    for t in range(2):
        load(dy, t, H.at[t], tile2_sem.at[t]).start()
    barrier = pltpu.get_barrier_semaphore()
    peers = [partner, ypeer, xpeer] + zpeer[1:]
    for dev in peers:
        pl.semaphore_signal(barrier, inc=1, device_id=dev, device_id_type=MESH)
    pl.semaphore_wait(barrier, len(peers))
    for d in own_copies(0):
        d.wait()
    R1(0)
    for d in own_copies(1):
        d.wait()
    for t in range(NT):
        load(x, t, DO.at[pl.ds(t * TM, TM)], tile_sem.at[t]).wait()
        load(dy, t, H.at[t % 2], tile2_sem.at[t % 2]).wait()

        def first(r, q):
            norm_rows(DO[r, :], r)
            ACC[r, :] = jnp.zeros_like(ACC[r, :])
            DOT[:, r] = H[t % 2, q, :].T
        pieces(t, first)
        if t + 2 < NT:
            load(dy, t + 2, H.at[t % 2], tile2_sem.at[t % 2]).start()
        if t == 0:
            R1(1)
        if t == 1:
            E(0)
            R1(2)
        if t == 3:
            E4(0)
    for d in a0_out():
        d.start()
    E(1)
    Ex(0)
    E4(1)

    def f0_chunk(i, _):
        E5(i)
        f0_step(i, 0)
        R1(i + 3)
        f0_step(i, 1)
        E(i + 2)
        f0_step(i, 2)
        Ex(i + 1)
        f0_step(i, 3)
        E4(i + 2)
        return 0

    lax.fori_loop(0, NJ, f0_chunk, 0)
    for d in a0_out():
        d.wait()

    for t in range(NT):
        def second(r, q):
            h = DO[r, :] + ACC[r, :].astype(bf)
            DO[r, :] = h
            ACC[r, :] = jnp.zeros_like(ACC[r, :])
            norm_rows(h, r)
        pieces(t, second)
        pltpu.make_async_copy(DO.at[pl.ds(t * TM, TM)], h1.at[pl.ds(t * TM, TM)], tile_sem.at[t]).start()
    for t in range(NT):
        pltpu.make_async_copy(DO.at[pl.ds(t * TM, TM)], h1.at[pl.ds(t * TM, TM)], tile_sem.at[t]).wait()
        load(dy, t, DO.at[pl.ds(t * TM, TM)], tile_sem.at[t]).start()
    for t in range(NT):
        load(dy, t, DO.at[pl.ds(t * TM, TM)], tile_sem.at[t]).wait()

    def layer_back(n, _):
        l = L - 1 - n

        def chunk(i, _):
            j = jmap(i)
            v = n * NJ + i
            u = NJ + i

            @pl.when(n == 0)
            def _():
                E5(u)
            wdt[...] = W[l, j].reshape(FC, D).T
            fwd(l, j, 0)

            @pl.when(i > 0)
            def _():
                A1S2(v - 1)
            wt[:FC] = weight(l, j, 0).T
            wt[FC:] = weight(l, j, 1).T
            bwd(l, j, 0)
            fwd(l, j, 1)

            @pl.when(v > 1)
            def _():
                A3(v - 2)

            @pl.when((n == 0) & (i == 0))
            def _():
                R1(2 * NJ - 1)

            @pl.when((n == 0) & (i < NJ - 2))
            def _():
                E(u + 2)
            bwd(l, j, 1)
            fwd(l, j, 2)

            @pl.when(v > 0)
            def _():
                A2S3(v - 1)
            bwd(l, j, 2)
            fwd(l, j, 3)

            @pl.when((n == 0) & (i < NJ - 2))
            def _():
                E4(u + 2)

            @pl.when((n == 0) & (i < NJ - 1))
            def _():
                Ex(u + 1)
            bwd(l, j, 3)
            S1(v)
            bwd_a(3)
            return 0

        lax.fori_loop(0, NJ, chunk, 0)

        def hload(t):
            return pltpu.make_async_copy(h1.at[pl.ds(t * TM, TM)], H.at[t % 2], tile2_sem.at[t % 2])

        def xload(t):
            return pltpu.make_async_copy(x.at[pl.ds(t * TM, TM)], H.at[t % 2], tile2_sem.at[t % 2])

        def start_h(t):
            @pl.when(n == 0)
            def _():
                hload(t).start()

            @pl.when(n == 1)
            def _():
                xload(t).start()

        start_h(0)
        start_h(1)

        @pl.when(n == 0)
        def _():
            for d in a0_in():
                d.start()
        for t in range(NT):
            xload(t).wait()
            def third(r, q):
                wide = H[t % 2, q, :].astype(f32)
                scale = scale_of(wide)
                g = ACC[r, :].astype(bf).astype(f32)
                m = jnp.mean(g * wide, -1, keepdims=True)
                back = (g * scale - wide * (scale * scale * scale * m)).astype(bf)
                o = DO[r, :] + back
                DO[r, :] = o
                ACC[r, :] = jnp.zeros_like(ACC[r, :])
                DOT[:, r] = o.T
            if t == 0:
                A1S2(n * NJ + NJ - 1)
            pieces(t, third)
            if t + 2 < NT:
                start_h(t + 2)

            @pl.when(n == 1)
            def _():
                pltpu.make_async_copy(DO.at[pl.ds(t * TM, TM)], dx.at[pl.ds(t * TM, TM)], tile_sem.at[t]).start()

        @pl.when(n == 0)
        def _():
            for d in a0_in():
                d.wait()
        return 0

    lax.fori_loop(0, L, layer_back, 0)
    last = L * NJ - 1
    A3(last - 1)
    A2S3(last)
    A3(last)
    for u in range(L * NJ):
        ag_finish(u)
    for d in s1(last) + s2(last):
        d.wait_send()
    s3_sent(last)
    for d in out_copies(last):
        d.wait()
    for l in range(L):
        outw(l).wait()
    for t in range(NT):
        pltpu.make_async_copy(DO.at[pl.ds(t * TM, TM)], dx.at[pl.ds(t * TM, TM)], tile_sem.at[t]).wait()


def hand_over(tiles, rows, *refs):
    src, dst, via, sem = refs[:4], refs[4:8], refs[8:12], refs[12]

    def part(ref, k, t):
        return ref[k].at[pl.ds(t * rows, rows)] if k == 0 else ref[k].at[t]

    into = [pltpu.make_async_copy(part(src, k, t), part(via, k, t), sem.at[n]) for n, (k, t) in enumerate(tiles)]
    out = [pltpu.make_async_copy(part(via, k, t), part(dst, k, t), sem.at[n]) for n, (k, t) in enumerate(tiles)]
    for d in into:
        d.start()
    for a, b in zip(into, out):
        a.wait()
        b.start()
    for d in out:
        d.wait()


def solution(mesh):
    def step(x, dy, wg, wu, wd):
        x, dy = x[0], dy[0]
        L, R, FF = wg.shape
        T, D = x.shape
        FR = wd.shape[1]
        FC = NJ * FR
        TM = T // NT
        V, S = pltpu.VMEM, pltpu.SemaphoreType.DMA
        scratch = [
            V((L, NJ, 2, Y, Z, C, R, FC), bf), V((L, NJ, Y, C, FR, D), bf),
            V((T, D), bf), V((D, T), bf), V((T, D), bf), V((D, T), bf), V((T, D), f32),
            V((Y, Z, C, R, FC), f32), V((Y, Z, C, R, FC), f32), V((D, FC), f32),
            V((2, TM, FC), bf), V((2, TM, 2 * FC), bf), V((2 * FC, D), bf), V((D, FC), bf),
            V((2, Y, Z, R, FC), bf), V((Y, FR, D), bf), V((2, 2, Y, Z, R, FC), bf), V((2, Y, FR, D), bf),
            V((2, Z, R, FC), bf), V((FR, D), bf), V((2, 2, Z, R, FC), bf), V((2, FR, D), bf),
            V((2, Z, R, FC), f32), V((FR, D), f32),
            V((4, 2, R, FC), bf), V((FR, D), bf), V((2, R, FC), f32), V((FR, D), f32),
            V((2, 3, 2, R, FC), bf), V((3, FR, D), bf), V((2, R, FC), bf), V((L, FR, D), bf),
            S((L, NJ * 4 + 1)), S((NT,)), S((2,)), S((L * NJ, 22)), S((L * NJ, 20)), S((8,)), S((2, 10)), S((4,)), S((L,)), S((2,)),
        ]
        any_ = pl.BlockSpec(memory_space=pl.ANY)
        dx, g, u, d, *_ = pl.pallas_call(
            kernel,
            out_shape=[jax.ShapeDtypeStruct(s, bf) for s in ((T, D), wg.shape, wu.shape, wd.shape, (T, D), (T, D), (D, T))],
            in_specs=[any_] * 5,
            out_specs=[any_] * 7,
            scratch_shapes=scratch,
            compiler_params=pltpu.CompilerParams(collective_id=0, has_side_effects=True, vmem_limit_bytes=67043328),
            name="stack",
        )(x, dy, wg, wu, wd)
        outs = (dx, g, u, d)
        tiles = [(k, t) for k in (1, 2, 3) for t in range(L)] + [(0, t) for t in range(16)]
        dx, g, u, d = pl.pallas_call(
            functools.partial(hand_over, tiles, T // 16),
            out_shape=[jax.ShapeDtypeStruct(t.shape, bf) for t in outs],
            in_specs=[any_] * 4,
            out_specs=[any_] * 4,
            scratch_shapes=[V(t.shape, bf) for t in outs] + [S((len(tiles),))],
            compiler_params=pltpu.CompilerParams(vmem_limit_bytes=67043328),
            cost_estimate=pl.CostEstimate(flops=0, bytes_accessed=10 * 2**20, transcendentals=0),
            name="hand_over",
        )(*outs)
        return dx[None], g, u, d

    w = P(None, "dp", None)
    t = P(("rep", "dp"), None, None)
    o = P("rep", "dp", None)
    return jax.shard_map(step, mesh=mesh, in_specs=(t, t, w, w, w), out_specs=(t, o, o, o), check_vma=False)
```
